32 devices in a mesh: row: 4 (over z), col: 8 (over y, x, core).
Axes of the slice: x: 2, y: 2, z: 4, core: 2. Of those that a mesh axis runs over, the one named last changes fastest.
Arguments:
- tokens: bfloat16 [24576, 256], P(('row', 'col'))
- codebook: bfloat16 [16384, 256], P(('row', 'col')), may hold values from -6 to 6
- codes: int32 [24576], P(('row', 'col')), may hold values from 0 to 16383
Outputs:
- quantized: bfloat16 [24576, 256], P(('row', 'col'))
- token_loss: float32 [24576], P(('row', 'col'))
- code_counts: int32 [16384], P(('row', 'col'))
- code_loss: float32 [16384], P(('row', 'col'))
- commitment: float32 [], replicated
- perplexity: float32 [], replicated
The draws below stay inside these ranges and needn't reach their ends.
All inputs are finite; a program needn't handle non-finite values.
Results may differ from the reference program's by a relative error of at most 0.0004.
Values may be sent and summed in bfloat16 or wider, within the bound.
A program may use at most 64 MiB of HBM per device.

```python
import math
import jax
import jax.numpy as jnp
import numpy as np

DIM = 256
CODES = 16384
TOKENS = 24576


def draw_tokens(key, part):
    key_norm = jax.random.fold_in(key, 11)
    key_scale = jax.random.fold_in(key, 12)
    values = jax.random.normal(key_norm, (TOKENS, DIM), jnp.float32)
    spread = jnp.exp(jax.random.uniform(key_scale, (TOKENS, 1), jnp.float32, jnp.log(0.2), jnp.log(2.0)))
    rising = 1.0 + 2.0 * jnp.arange(TOKENS, dtype=jnp.float32)[:, None] / TOKENS
    return (values * spread * rising).astype(jnp.bfloat16)


def touch_ends(drawn, own_key, smallest, top_value):
    index_at = [jax.random.randint(jax.random.fold_in(own_key, axis), (), 0, length) for axis, length in enumerate(drawn.shape)]
    main_axis = drawn.shape.index(max(drawn.shape))
    next_to = index_at[:main_axis] + [(index_at[main_axis] + 1) % drawn.shape[main_axis]] + index_at[main_axis + 1:]
    return drawn.at[tuple(index_at)].set(smallest).at[tuple(next_to)].set(top_value)


def levels(rng, extent, cuts, low, top_value):
    def one(position, shards_of):
        draws = jax.random.uniform(jax.random.fold_in(jax.random.fold_in(rng, 6), position), (shards_of,), jnp.float32, low / len(cuts), top_value / len(cuts))
        return jnp.repeat(jnp.exp(draws), extent[position] // shards_of).reshape((-1,) + (1,) * (len(extent) - position - 1))

    level = one(*cuts[0])
    for cut in cuts[1:]:
        level = level * one(*cut)
    return level


def rank_bounds(amount, lean):
    portions = [(1 << 20) // math.isqrt(rank ** lean) + 1 for rank in range(1, amount + 1)]
    scale = 1 + sum(portions) // (1 << 30)
    return np.cumsum(np.array([max(1, weight // scale) for weight in portions]))


def ranked(own_key, extent, count, lean):
    listing = rank_bounds(count, lean)
    lot = jax.random.randint(jax.random.fold_in(own_key, 1), extent, 0, int(listing[count - 1]))
    rank = jnp.searchsorted(jnp.asarray(listing, jnp.int32), lot, side="right")
    return jax.random.permutation(jax.random.fold_in(own_key, 2), count)[rank].astype(jnp.int32)


def normal_values(stream_key, shape, scale, most, cuts=(), kind=jnp.bfloat16):
    loudness = levels(stream_key, shape, cuts, -0.22, 0.18) if cuts else 1.0
    entries = jax.random.normal(stream_key, shape, jnp.float32) * scale * loudness
    return jnp.minimum(jnp.maximum(entries, -most), most).astype(kind)


def setup_inputs(seed: int = 0) -> dict:
    seeds = jax.random.split(jax.random.key(seed), 4)
    tokens = draw_tokens(jax.random.fold_in(seeds[3], 71), 0)
    codebook = normal_values(seeds[1], (CODES, DIM), 1.0, 6.0, ((0, 32),))
    codes = touch_ends(ranked(seeds[2], (TOKENS,), CODES, 2), jax.random.fold_in(seeds[2], 3), 0, CODES - 1).astype(jnp.int32)
    return dict(tokens=tokens, codebook=codebook, codes=codes)


def reference(tokens, codebook, codes):
    quantized = jnp.take(codebook, codes, axis=0)
    diff = tokens.astype(jnp.float32) - quantized.astype(jnp.float32)
    token_loss = jnp.sum(diff * diff, axis=1) / DIM
    code_counts = jnp.zeros((CODES,), jnp.int32).at[codes].add(1)
    code_loss = jax.ops.segment_sum(token_loss, codes, num_segments=CODES)
    commitment = 0.25 * jnp.sum(token_loss) / TOKENS
    probs = code_counts.astype(jnp.float32) / TOKENS
    floor_prob = jnp.float32(1.0 / TOKENS)
    terms = jnp.where(code_counts > 0, probs * jnp.log(jnp.maximum(probs, floor_prob)), jnp.float32(0.0))
    perplexity = jnp.exp(-jnp.sum(terms))
    return quantized, token_loss, code_counts, code_loss, commitment, perplexity
```

```python
import functools
import math

import jax
import jax.numpy as jnp
from jax import lax
from jax.experimental import pallas as pl
from jax.experimental.pallas import tpu as pltpu
from jax.sharding import PartitionSpec as P

AXES = ("row", "col")
EXTRA = 128
F32 = jnp.float32
BF16 = jnp.bfloat16


def dense_plan(tokens, codebook, codes):
    tok_rows = tokens.shape[0]
    width = tokens.shape[1]
    per_dev = codebook.shape[0]
    devices = lax.axis_size("row") * lax.axis_size("col")
    total_codes = per_dev * devices
    total_tokens = tok_rows * devices
    full_book = lax.all_gather(codebook, AXES, axis=0, tiled=True)
    quantized = jnp.take(full_book, codes, axis=0)
    diff = tokens.astype(F32) - quantized.astype(F32)
    token_loss = jnp.sum(diff * diff, axis=1) / width
    loss_part = jnp.sum(token_loss)
    local_counts = jax.ops.segment_sum(
        jnp.ones((tok_rows,), F32), codes, num_segments=total_codes
    )
    local_loss = jax.ops.segment_sum(token_loss, codes, num_segments=total_codes)
    floor_prob = jnp.float32(1.0 / total_tokens)
    totals, loss_totals = lax.psum((local_counts, local_loss), AXES)
    loss_sum = lax.psum(loss_part, AXES)
    probs = totals / total_tokens
    terms = jnp.where(
        totals > 0.5, probs * jnp.log(jnp.maximum(probs, floor_prob)), jnp.float32(0.0)
    )
    offset = lax.axis_index(AXES) * per_dev
    owned_counts = lax.dynamic_slice_in_dim(totals, offset, per_dev, 0)
    code_loss = lax.dynamic_slice_in_dim(loss_totals, offset, per_dev, 0)
    commitment = 0.25 * loss_sum / total_tokens
    return (
        quantized,
        token_loss,
        owned_counts.astype(jnp.int32),
        code_loss,
        commitment,
        jnp.exp(-jnp.sum(terms)),
    )


def ring_plan(n, tokens, codebook, codes):
    rows, width = tokens.shape
    per_dev = codebook.shape[0]
    me = lax.axis_index(AXES)
    ring = [(i, (i + 1) % n) for i in range(n)]
    hi = codes // per_dev
    lo = codes % per_dev

    def pick(step, carry):
        block, got = carry
        owner = lax.rem(me - step + n, n)
        got = jnp.where((hi == owner)[:, None], jnp.take(block, lo, axis=0), got)
        return lax.ppermute(block, AXES, ring), got

    _, quantized = lax.fori_loop(0, n, pick, (codebook, jnp.zeros_like(tokens)))
    diff = tokens.astype(F32) - quantized.astype(F32)
    token_loss = jnp.sum(diff * diff, axis=1) / width

    def add(step, carry):
        c, t, total, parts = carry
        owner = lax.rem(me - step + n, n)
        mine = (c // per_dev) == me
        total = total + jax.ops.segment_sum(
            jnp.where(mine, t, 0.0), c % per_dev, num_segments=per_dev
        )
        parts = lax.dynamic_update_slice(parts, jnp.sum(t)[None], (owner,))
        return lax.ppermute(c, AXES, ring), lax.ppermute(t, AXES, ring), total, parts

    start = (codes, token_loss, jnp.zeros((per_dev,), F32), jnp.zeros((n,), F32))
    _, _, code_loss, parts = lax.fori_loop(0, n, add, start)
    return quantized, token_loss, code_loss, 0.25 * jnp.sum(parts) / (rows * n)


def kernel(
    n, cols, cap, stride,
    codes_ref, tokens_ref, book_ref,
    quant_ref, tloss_ref, counts_ref, closs_ref, commit_ref, perp_ref, flag_ref,
    csend, crecv, psend, precv, lsend, lrecv, ranks, low1h, sel,
    csem_s, csem_r, psem_s, psem_r, lsem_s, lsem_r,
):
    rows, width = tokens_ref.shape
    per = book_ref.shape[0]
    bits = per.bit_length() - 1
    total_tokens = rows * n
    me = lax.axis_index("row") * cols + lax.axis_index("col")

    def where_is(r):
        return (r // cols, lax.rem(r, cols))

    def peer(k):
        return lax.rem(me + lax.rem(k * stride, n), n)

    def copy(send, recv, ssem, rsem, r):
        return pltpu.make_async_remote_copy(
            src_ref=send.at[r],
            dst_ref=recv.at[me],
            send_sem=ssem.at[r],
            recv_sem=rsem.at[me],
            device_id=where_is(r),
            device_id_type=pl.DeviceIdType.MESH,
        )

    def arrived(send, recv, ssem, rsem, r):
        pltpu.make_async_remote_copy(
            src_ref=send.at[r],
            dst_ref=recv.at[r],
            send_sem=ssem.at[r],
            recv_sem=rsem.at[r],
            device_id=where_is(r),
            device_id_type=pl.DeviceIdType.MESH,
        ).wait_recv()

    def each_peer(fn):
        def body(k, _):
            fn(peer(k))
            return 0

        lax.fori_loop(1, n, body, 0)

    barrier = pltpu.get_barrier_semaphore()
    each_peer(
        lambda r: pl.semaphore_signal(
            barrier, inc=1, device_id=where_is(r), device_id_type=pl.DeviceIdType.MESH
        )
    )

    code_row = codes_ref[...]
    hi_row = lax.shift_right_logical(code_row, bits)
    code_col = jnp.broadcast_to(code_row.astype(F32), (128, rows)).T.astype(jnp.int32)
    hi_col = lax.shift_right_logical(code_col, bits)
    lo_col = code_col & (per - 1)
    lane = lax.broadcasted_iota(jnp.int32, (rows, 128), 1)
    own_row = hi_row == lax.broadcasted_iota(jnp.int32, (n, rows), 0)
    for k in range(per // 128):
        low1h[:, k * 128 : (k + 1) * 128] = jnp.where(lo_col == lane + k * 128, 1.0, 0.0).astype(BF16)
    low = low1h[...]
    hist = jnp.dot(jnp.where(own_row, 1.0, 0.0).astype(BF16), low, preferred_element_type=F32)
    wanted = jnp.where(hist > 0.5, 1.0, 0.0)
    most = jnp.max(jnp.sum(wanted, axis=1, keepdims=True), axis=0, keepdims=True)
    most_wide = jnp.broadcast_to(most, (1, EXTRA))
    for p in range(n):
        csend[p, :, :per] = hist[p : p + 1, :]
        csend[p, :, per:] = most_wide
    crecv[pl.ds(me, 1)] = csend[pl.ds(me, 1)]

    pl.semaphore_wait(barrier, n - 1)
    each_peer(lambda r: copy(csend, crecv, csem_s, csem_r, r).start())

    before = lax.broadcasted_iota(jnp.int32, (per, per), 0) < lax.broadcasted_iota(jnp.int32, (per, per), 1)
    before = jnp.where(before, 1.0, 0.0).astype(BF16)
    rank = jnp.dot(wanted.astype(BF16), before, preferred_element_type=F32)
    rank = jnp.minimum(rank, 255.0).astype(BF16)
    hi1h = jnp.where(hi_col[:, :n] == lane[:, :n], 1.0, 0.0).astype(BF16)
    looked = jnp.dot(hi1h, rank, preferred_element_type=F32).astype(BF16) * low
    found = jnp.dot(looked, jnp.ones((per, 128), BF16), preferred_element_type=F32)
    slot = hi_col * cap + found.astype(jnp.int32)
    for k in range(n * cap // 128):
        sel[:, k * 128 : (k + 1) * 128] = jnp.where(slot == lane + k * 128, 1.0, 0.0).astype(BF16)

    each_peer(lambda r: arrived(csend, crecv, csem_s, csem_r, r))
    asked = crecv[:, 0, :per]
    present = asked > 0.5
    order = jnp.dot(jnp.where(present, 1.0, 0.0).astype(BF16), before, preferred_element_type=F32)
    order = jnp.where(present, order, -1.0)
    for p in range(n):
        ranks[p] = order[p : p + 1, :]

    place = lax.broadcasted_iota(jnp.int32, (cap, per), 0).astype(F32)

    def pack(r):
        picks = jnp.where(jnp.broadcast_to(ranks[r], (cap, per)) == place, 1.0, 0.0).astype(BF16)
        return jnp.dot(picks, book_ref[...], preferred_element_type=F32).astype(BF16)

    def pack_and_send(k, _):
        r = peer(k)
        psend[r] = pack(r)

        @pl.when(k > 1)
        def _():
            copy(psend, precv, psem_s, psem_r, peer(k - 1)).start()

        return 0

    lax.fori_loop(1, n, pack_and_send, 0)
    precv[me] = pack(me)
    copy(psend, precv, psem_s, psem_r, peer(n - 1)).start()

    counts = jnp.sum(asked, axis=0, keepdims=True)
    counts_ref[...] = counts.astype(jnp.int32)
    probs = counts / total_tokens
    terms = jnp.where(
        counts > 0.5, probs * jnp.log(jnp.maximum(probs, 1.0 / total_tokens)), 0.0
    )
    entropy = jnp.sum(terms, axis=1, keepdims=True)
    flag_ref[0, 0] = jnp.max(crecv[:, 0, per:]).astype(jnp.int32)

    each_peer(lambda r: arrived(psend, precv, psem_s, psem_r, r))
    packs = precv[...].reshape(n * cap, width)
    quant = jnp.dot(sel[...], packs, preferred_element_type=F32).astype(BF16)
    quant_ref[...] = quant
    diff = tokens_ref[...].astype(F32) - quant.astype(F32)
    square = diff * diff
    folded = square[:, :128]
    for k in range(1, width // 128):
        folded = folded + square[:, k * 128 : (k + 1) * 128]
    tloss = jnp.sum(folded.T, axis=0, keepdims=True) / width
    tloss_ref[...] = tloss
    part = jnp.sum(tloss, axis=1, keepdims=True)

    first = tloss.astype(BF16).astype(F32)
    second = (tloss - first).astype(BF16).astype(F32)
    third = tloss - first - second
    spread = jnp.concatenate(
        [jnp.where(own_row, x, 0.0).astype(BF16) for x in (first, second, third)], axis=0
    )
    sums = jnp.dot(spread, low1h[...], preferred_element_type=F32)
    sums = sums[:n] + sums[n : 2 * n] + sums[2 * n :]
    lane1 = lax.broadcasted_iota(jnp.int32, (1, EXTRA), 1)
    tail = jnp.where(lane1 == 0, part, jnp.where(lane1 == 1, entropy, 0.0))
    for p in range(n):
        lsend[p, :, :per] = sums[p : p + 1, :]
        lsend[p, :, per:] = tail
    lrecv[pl.ds(me, 1)] = lsend[pl.ds(me, 1)]
    each_peer(lambda r: copy(lsend, lrecv, lsem_s, lsem_r, r).start())

    def sent(r):
        copy(csend, crecv, csem_s, csem_r, r).wait_send()
        copy(psend, precv, psem_s, psem_r, r).wait_send()

    each_peer(sent)
    each_peer(lambda r: arrived(lsend, lrecv, lsem_s, lsem_r, r))
    added = jnp.sum(lrecv[:, 0, :], axis=0, keepdims=True)
    closs_ref[...] = added[:, :per]
    ends = added[:, per:]
    commit_ref[0, 0] = jnp.sum(jnp.where(lane1 == 0, ends, 0.0)) * (0.25 / total_tokens)
    perp = jnp.exp(-jnp.sum(jnp.where(lane1 == 1, ends, 0.0), axis=1, keepdims=True))
    perp_ref[0, 0] = jnp.max(jnp.broadcast_to(perp, (1, EXTRA)))
    each_peer(lambda r: copy(lsend, lrecv, lsem_s, lsem_r, r).wait_send())


def asked_plan(n, cols, tokens, codebook, codes):
    rows, width = tokens.shape
    per = codebook.shape[0]
    cap = -(-2 * rows // (n * 16)) * 16
    stride = next(s for s in range(n // 3 + 1, 2 * n) if math.gcd(s, n) == 1)
    vmem = pl.BlockSpec(memory_space=pltpu.VMEM)
    smem = pl.BlockSpec(memory_space=pltpu.SMEM)
    dma = pltpu.SemaphoreType.DMA((n,))
    message = pltpu.VMEM((n, 1, per + EXTRA), F32)
    quantized, token_loss, counts, code_loss, commitment, perplexity, flag = pl.pallas_call(
        functools.partial(kernel, n, cols, cap, stride),
        out_shape=(
            jax.ShapeDtypeStruct((rows, width), BF16),
            jax.ShapeDtypeStruct((1, rows), F32),
            jax.ShapeDtypeStruct((1, per), jnp.int32),
            jax.ShapeDtypeStruct((1, per), F32),
            jax.ShapeDtypeStruct((1, 1), F32),
            jax.ShapeDtypeStruct((1, 1), F32),
            jax.ShapeDtypeStruct((1, 1), jnp.int32),
        ),
        in_specs=[vmem] * 3,
        out_specs=(vmem, vmem, vmem, vmem, smem, smem, smem),
        scratch_shapes=[
            message, message,
            pltpu.VMEM((n, cap, width), BF16),
            pltpu.VMEM((n, cap, width), BF16),
            message, message,
            pltpu.VMEM((n, 1, per), F32),
            pltpu.VMEM((rows, per), BF16),
            pltpu.VMEM((rows, n * cap), BF16),
            dma, dma, dma, dma, dma, dma,
        ],
        compiler_params=pltpu.CompilerParams(collective_id=0, has_side_effects=True),
    )(codes.reshape(1, rows), tokens, codebook)

    def kept():
        return quantized, token_loss.reshape(rows), code_loss.reshape(per), commitment[0, 0]

    quantized, token_loss, code_loss, commitment = lax.cond(
        flag[0, 0] > cap, lambda: ring_plan(n, tokens, codebook, codes), kept
    )
    return (
        quantized,
        token_loss,
        counts.reshape(per),
        code_loss,
        commitment,
        perplexity[0, 0],
    )


def on_device(n, cols, tokens, codebook, codes):
    rows, width = tokens.shape
    per = codebook.shape[0]
    cap = -(-2 * rows // (n * 16)) * 16
    fits = (
        per % 128 == 0
        and per & (per - 1) == 0
        and rows % 128 == 0
        and width % 128 == 0
        and n * cap % 128 == 0
        and n % 8 == 0
        and n <= 128
        and cap < min(per, 256)
    )
    if fits:
        return asked_plan(n, cols, tokens, codebook, codes)
    return dense_plan(tokens, codebook, codes)


def solution(mesh):
    n = mesh.shape["row"] * mesh.shape["col"]
    return jax.shard_map(
        functools.partial(on_device, n, mesh.shape["col"]),
        mesh=mesh,
        in_specs=(P(AXES, None), P(AXES, None), P(AXES)),
        out_specs=(P(AXES, None), P(AXES), P(AXES), P(AXES), P(), P()),
        check_vma=False,
    )
```

```python
import functools

import jax
import jax.numpy as jnp
from jax import lax
from jax.experimental import pallas as pl
from jax.experimental.pallas import tpu as pltpu
from jax.sharding import PartitionSpec as P

AXES = ("row", "col")
EXTRA = 128
GROUP = 4
F32 = jnp.float32
BF16 = jnp.bfloat16


def dense_plan(tokens, codebook, codes):
    tok_rows = tokens.shape[0]
    width = tokens.shape[1]
    per_dev = codebook.shape[0]
    devices = lax.axis_size("row") * lax.axis_size("col")
    total_codes = per_dev * devices
    total_tokens = tok_rows * devices
    full_book = lax.all_gather(codebook, AXES, axis=0, tiled=True)
    quantized = jnp.take(full_book, codes, axis=0)
    diff = tokens.astype(F32) - quantized.astype(F32)
    token_loss = jnp.sum(diff * diff, axis=1) / width
    loss_part = jnp.sum(token_loss)
    local_counts = jax.ops.segment_sum(
        jnp.ones((tok_rows,), F32), codes, num_segments=total_codes
    )
    local_loss = jax.ops.segment_sum(token_loss, codes, num_segments=total_codes)
    floor_prob = jnp.float32(1.0 / total_tokens)
    totals, loss_totals = lax.psum((local_counts, local_loss), AXES)
    loss_sum = lax.psum(loss_part, AXES)
    probs = totals / total_tokens
    terms = jnp.where(
        totals > 0.5, probs * jnp.log(jnp.maximum(probs, floor_prob)), jnp.float32(0.0)
    )
    offset = lax.axis_index(AXES) * per_dev
    owned_counts = lax.dynamic_slice_in_dim(totals, offset, per_dev, 0)
    code_loss = lax.dynamic_slice_in_dim(loss_totals, offset, per_dev, 0)
    commitment = 0.25 * loss_sum / total_tokens
    return (
        quantized,
        token_loss,
        owned_counts.astype(jnp.int32),
        code_loss,
        commitment,
        jnp.exp(-jnp.sum(terms)),
    )


def ring_plan(n, tokens, codebook, codes):
    rows, width = tokens.shape
    per_dev = codebook.shape[0]
    me = lax.axis_index(AXES)
    ring = [(i, (i + 1) % n) for i in range(n)]
    hi = codes // per_dev
    lo = codes % per_dev

    def pick(step, carry):
        block, got = carry
        owner = lax.rem(me - step + n, n)
        got = jnp.where((hi == owner)[:, None], jnp.take(block, lo, axis=0), got)
        return lax.ppermute(block, AXES, ring), got

    _, quantized = lax.fori_loop(0, n, pick, (codebook, jnp.zeros_like(tokens)))
    diff = tokens.astype(F32) - quantized.astype(F32)
    token_loss = jnp.sum(diff * diff, axis=1) / width

    def add(step, carry):
        c, t, total, parts = carry
        owner = lax.rem(me - step + n, n)
        mine = (c // per_dev) == me
        total = total + jax.ops.segment_sum(
            jnp.where(mine, t, 0.0), c % per_dev, num_segments=per_dev
        )
        parts = lax.dynamic_update_slice(parts, jnp.sum(t)[None], (owner,))
        return lax.ppermute(c, AXES, ring), lax.ppermute(t, AXES, ring), total, parts

    start = (codes, token_loss, jnp.zeros((per_dev,), F32), jnp.zeros((n,), F32))
    _, _, code_loss, parts = lax.fori_loop(0, n, add, start)
    return quantized, token_loss, code_loss, 0.25 * jnp.sum(parts) / (rows * n)


def kernel(
    n, cols, cap, order_of,
    codes_ref, tokens_ref, book_ref,
    quant_ref, tloss_ref, counts_ref, closs_ref, commit_ref, perp_ref, flag_ref,
    csend, crecv, psend, precv, lsend, lrecv, ranks, low1h, sel,
    csem_s, csem_r, psem_s, psem_r, lsem_s, lsem_r,
):
    rows, width = tokens_ref.shape
    per = book_ref.shape[0]
    bits = per.bit_length() - 1
    total_tokens = rows * n
    my_row, my_col = lax.axis_index("row"), lax.axis_index("col")
    me = my_row * cols + my_col
    rows_at = [lax.rem(my_row + d, n // cols) for d in range(n // cols)]
    cols_at = [lax.rem(my_col + d, cols) for d in range(cols)]
    at = [(rows_at[k // cols], cols_at[k % cols]) for k in range(n)]
    peer = [r * cols + c for r, c in at]

    def copy(send, recv, ssem, rsem, k):
        return pltpu.make_async_remote_copy(
            src_ref=send.at[peer[k]],
            dst_ref=recv.at[me],
            send_sem=ssem.at[k],
            recv_sem=rsem.at[k],
            device_id=at[k],
            device_id_type=pl.DeviceIdType.MESH,
        )

    def start_all(*refs):
        for k in order_of:
            if k:
                copy(*refs, k).start()

    def wait_all(*refs):
        for k in order_of:
            if k:
                copy(*refs, k).wait_recv()

    def sent_all(*refs):
        for k in order_of:
            if k:
                copy(*refs, k).wait_send()

    barrier = pltpu.get_barrier_semaphore()
    for k in order_of:
        if k:
            pl.semaphore_signal(
                barrier, inc=1, device_id=at[k], device_id_type=pl.DeviceIdType.MESH
            )

    code_row = codes_ref[...]
    hi_row = lax.shift_right_logical(code_row, bits)
    code_col = jnp.broadcast_to(code_row.astype(F32), (128, rows)).T.astype(jnp.int32)
    hi_col = lax.shift_right_logical(code_col, bits)
    lo_col = code_col & (per - 1)
    lane = lax.broadcasted_iota(jnp.int32, (rows, 128), 1)
    own_row = hi_row == lax.broadcasted_iota(jnp.int32, (n, rows), 0)
    for k in range(per // 128):
        low1h[:, k * 128 : (k + 1) * 128] = jnp.where(lo_col == lane + k * 128, 1.0, 0.0).astype(BF16)
    low = low1h[...]
    hist = jnp.dot(jnp.where(own_row, 1.0, 0.0).astype(BF16), low, preferred_element_type=F32)
    wanted = jnp.where(hist > 0.5, 1.0, 0.0)
    most = jnp.max(jnp.sum(wanted, axis=1, keepdims=True), axis=0, keepdims=True)
    most_wide = jnp.broadcast_to(most, (1, EXTRA))
    for p in range(n):
        csend[p, :, :per] = hist[p : p + 1, :]
        csend[p, :, per:] = most_wide
    crecv[pl.ds(me, 1)] = csend[pl.ds(me, 1)]

    pl.semaphore_wait(barrier, n - 1)
    start_all(csend, crecv, csem_s, csem_r)

    before = lax.broadcasted_iota(jnp.int32, (per, per), 0) < lax.broadcasted_iota(jnp.int32, (per, per), 1)
    before = jnp.where(before, 1.0, 0.0).astype(BF16)
    rank = jnp.dot(wanted.astype(BF16), before, preferred_element_type=F32)
    rank = jnp.minimum(rank, 255.0).astype(BF16)
    hi1h = jnp.where(hi_col[:, :n] == lane[:, :n], 1.0, 0.0).astype(BF16)
    looked = jnp.dot(hi1h, rank, preferred_element_type=F32).astype(BF16) * low
    found = jnp.dot(looked, jnp.ones((per, 128), BF16), preferred_element_type=F32)
    slot = hi_col * cap + found.astype(jnp.int32)
    for k in range(n * cap // 128):
        sel[:, k * 128 : (k + 1) * 128] = jnp.where(slot == lane + k * 128, 1.0, 0.0).astype(BF16)

    wait_all(csend, crecv, csem_s, csem_r)
    asked = crecv[:, 0, :per]
    present = asked > 0.5
    order = jnp.dot(jnp.where(present, 1.0, 0.0).astype(BF16), before, preferred_element_type=F32)
    order = jnp.where(present, order, -1.0)
    for p in range(n):
        ranks[p] = order[p : p + 1, :]

    place = lax.broadcasted_iota(jnp.int32, (cap, per), 0).astype(F32)
    book = book_ref[...]
    ready = []
    for g in range(0, n, GROUP):
        group = order_of[g : g + GROUP]
        picks = [
            jnp.where(jnp.broadcast_to(ranks[peer[k]], (cap, per)) == place, 1.0, 0.0).astype(BF16)
            for k in group
        ]
        packed = jnp.dot(jnp.concatenate(picks, axis=0), book, preferred_element_type=F32)
        packed = packed.astype(BF16)
        for i, k in enumerate(group):
            out = psend if k else precv
            out[peer[k]] = packed[i * cap : (i + 1) * cap]
        for k in ready:
            copy(psend, precv, psem_s, psem_r, k).start()
        ready = [k for k in group if k]
    for k in ready:
        copy(psend, precv, psem_s, psem_r, k).start()

    counts = jnp.sum(asked, axis=0, keepdims=True)
    counts_ref[...] = counts.astype(jnp.int32)
    probs = counts / total_tokens
    terms = jnp.where(
        counts > 0.5, probs * jnp.log(jnp.maximum(probs, 1.0 / total_tokens)), 0.0
    )
    entropy = jnp.sum(terms, axis=1, keepdims=True)
    flag_ref[0, 0] = jnp.max(crecv[:, 0, per:]).astype(jnp.int32)

    wait_all(psend, precv, psem_s, psem_r)
    packs = precv[...].reshape(n * cap, width)
    quant = jnp.dot(sel[...], packs, preferred_element_type=F32).astype(BF16)
    quant_ref[...] = quant
    diff = tokens_ref[...].astype(F32) - quant.astype(F32)
    square = diff * diff
    folded = square[:, :128]
    for k in range(1, width // 128):
        folded = folded + square[:, k * 128 : (k + 1) * 128]
    tloss = jnp.sum(folded.T, axis=0, keepdims=True) / width
    tloss_ref[...] = tloss
    part = jnp.sum(tloss, axis=1, keepdims=True)

    first = tloss.astype(BF16).astype(F32)
    second = (tloss - first).astype(BF16).astype(F32)
    third = tloss - first - second
    spread = jnp.concatenate(
        [jnp.where(own_row, x, 0.0).astype(BF16) for x in (first, second, third)], axis=0
    )
    sums = jnp.dot(spread, low1h[...], preferred_element_type=F32)
    sums = sums[:n] + sums[n : 2 * n] + sums[2 * n :]
    lane1 = lax.broadcasted_iota(jnp.int32, (1, EXTRA), 1)
    tail = jnp.where(lane1 == 0, part, jnp.where(lane1 == 1, entropy, 0.0))
    for p in range(n):
        lsend[p, :, :per] = sums[p : p + 1, :]
        lsend[p, :, per:] = tail
    lrecv[pl.ds(me, 1)] = lsend[pl.ds(me, 1)]
    start_all(lsend, lrecv, lsem_s, lsem_r)

    sent_all(csend, crecv, csem_s, csem_r)
    sent_all(psend, precv, psem_s, psem_r)
    wait_all(lsend, lrecv, lsem_s, lsem_r)
    added = jnp.sum(lrecv[:, 0, :], axis=0, keepdims=True)
    closs_ref[...] = added[:, :per]
    ends = added[:, per:]
    commit_ref[0, 0] = jnp.sum(jnp.where(lane1 == 0, ends, 0.0)) * (0.25 / total_tokens)
    perp = jnp.exp(-jnp.sum(jnp.where(lane1 == 1, ends, 0.0), axis=1, keepdims=True))
    perp_ref[0, 0] = jnp.max(jnp.broadcast_to(perp, (1, EXTRA)))
    sent_all(lsend, lrecv, lsem_s, lsem_r)


def send_order(n, cols):
    turns = sorted(range(n // cols), key=lambda d: (abs(2 * d - n // cols), d))
    turns = [d for d in turns if d] + [0]
    blocks = [(d, h) for d in turns for h in (0, 1)]
    half = cols // 2
    spread = sorted(blocks[2:-2], key=lambda b: b[1])
    blocks = blocks[:2] + spread + [(0, 1), (0, 0)]
    return [d * cols + h * half + c for d, h in blocks for c in range(half)]


def exchange(n, cols, cap, number, tokens, codebook, codes):
    rows, width = tokens.shape
    per = codebook.shape[0]
    vmem = pl.BlockSpec(memory_space=pltpu.VMEM)
    smem = pl.BlockSpec(memory_space=pltpu.SMEM)
    dma = pltpu.SemaphoreType.DMA((n,))
    message = pltpu.VMEM((n, 1, per + EXTRA), F32)
    return pl.pallas_call(
        functools.partial(kernel, n, cols, cap, send_order(n, cols)),
        out_shape=(
            jax.ShapeDtypeStruct((rows, width), BF16),
            jax.ShapeDtypeStruct((1, rows), F32),
            jax.ShapeDtypeStruct((1, per), jnp.int32),
            jax.ShapeDtypeStruct((1, per), F32),
            jax.ShapeDtypeStruct((1, 1), F32),
            jax.ShapeDtypeStruct((1, 1), F32),
            jax.ShapeDtypeStruct((1, 1), jnp.int32),
        ),
        in_specs=[vmem] * 3,
        out_specs=(vmem, vmem, vmem, vmem, smem, smem, smem),
        scratch_shapes=[
            message, message,
            pltpu.VMEM((n, cap, width), BF16),
            pltpu.VMEM((n, cap, width), BF16),
            message, message,
            pltpu.VMEM((n, 1, per), F32),
            pltpu.VMEM((rows, per), BF16),
            pltpu.VMEM((rows, n * cap), BF16),
            dma, dma, dma, dma, dma, dma,
        ],
        compiler_params=pltpu.CompilerParams(collective_id=number, has_side_effects=True),
    )(codes, tokens, codebook)


def asked_plan(n, cols, cap, tokens, codebook, codes):
    rows = tokens.shape[0]
    per = codebook.shape[0]
    code_row = codes.reshape(1, rows)
    quantized, token_loss, counts, code_loss, commitment, perplexity, flag = exchange(
        n, cols, cap, 0, tokens, codebook, code_row
    )

    def kept():
        return quantized, token_loss.reshape(rows), code_loss.reshape(per), commitment[0, 0]

    def wider():
        q, t, _, c, m, _, _ = exchange(n, cols, 2 * cap, 1, tokens, codebook, code_row)
        return q, t.reshape(rows), c.reshape(per), m[0, 0]

    def any_codes():
        return lax.cond(
            flag[0, 0] > 2 * cap, lambda: ring_plan(n, tokens, codebook, codes), wider
        )

    quantized, token_loss, code_loss, commitment = lax.cond(flag[0, 0] > cap, any_codes, kept)
    return (
        quantized,
        token_loss,
        counts.reshape(per),
        code_loss,
        commitment,
        perplexity[0, 0],
    )


def on_device(n, cols, tokens, codebook, codes):
    rows, width = tokens.shape
    per = codebook.shape[0]
    cap = -(-rows // (n * 16)) * 16
    fits = (
        per % 128 == 0
        and per & (per - 1) == 0
        and rows % 128 == 0
        and width % 128 == 0
        and n * cap % 128 == 0
        and cols % 8 == 0
        and n // cols > 1
        and n <= 128
        and 2 * cap < min(per, 256)
    )
    if fits:
        return asked_plan(n, cols, cap, tokens, codebook, codes)
    return dense_plan(tokens, codebook, codes)


def solution(mesh):
    n = mesh.shape["row"] * mesh.shape["col"]
    return jax.shard_map(
        functools.partial(on_device, n, mesh.shape["col"]),
        mesh=mesh,
        in_specs=(P(AXES, None), P(AXES, None), P(AXES)),
        out_specs=(P(AXES, None), P(AXES), P(AXES), P(AXES), P(), P()),
        check_vma=False,
    )
```

```python
import functools

import jax
import jax.numpy as jnp
from jax import lax
from jax.experimental import pallas as pl
from jax.experimental.pallas import tpu as pltpu
from jax.sharding import PartitionSpec as P

AXES = ("row", "col")
EXTRA = 128
GROUP = 4
F32 = jnp.float32
BF16 = jnp.bfloat16


def dense_plan(tokens, codebook, codes):
    tok_rows = tokens.shape[0]
    width = tokens.shape[1]
    per_dev = codebook.shape[0]
    devices = lax.axis_size("row") * lax.axis_size("col")
    total_codes = per_dev * devices
    total_tokens = tok_rows * devices
    full_book = lax.all_gather(codebook, AXES, axis=0, tiled=True)
    quantized = jnp.take(full_book, codes, axis=0)
    diff = tokens.astype(F32) - quantized.astype(F32)
    token_loss = jnp.sum(diff * diff, axis=1) / width
    loss_part = jnp.sum(token_loss)
    local_counts = jax.ops.segment_sum(
        jnp.ones((tok_rows,), F32), codes, num_segments=total_codes
    )
    local_loss = jax.ops.segment_sum(token_loss, codes, num_segments=total_codes)
    floor_prob = jnp.float32(1.0 / total_tokens)
    totals, loss_totals = lax.psum((local_counts, local_loss), AXES)
    loss_sum = lax.psum(loss_part, AXES)
    probs = totals / total_tokens
    terms = jnp.where(
        totals > 0.5, probs * jnp.log(jnp.maximum(probs, floor_prob)), jnp.float32(0.0)
    )
    offset = lax.axis_index(AXES) * per_dev
    owned_counts = lax.dynamic_slice_in_dim(totals, offset, per_dev, 0)
    code_loss = lax.dynamic_slice_in_dim(loss_totals, offset, per_dev, 0)
    commitment = 0.25 * loss_sum / total_tokens
    return (
        quantized,
        token_loss,
        owned_counts.astype(jnp.int32),
        code_loss,
        commitment,
        jnp.exp(-jnp.sum(terms)),
    )


def ring_plan(n, tokens, codebook, codes):
    rows, width = tokens.shape
    per_dev = codebook.shape[0]
    me = lax.axis_index(AXES)
    ring = [(i, (i + 1) % n) for i in range(n)]
    hi = codes // per_dev
    lo = codes % per_dev

    def pick(step, carry):
        block, got = carry
        owner = lax.rem(me - step + n, n)
        got = jnp.where((hi == owner)[:, None], jnp.take(block, lo, axis=0), got)
        return lax.ppermute(block, AXES, ring), got

    _, quantized = lax.fori_loop(0, n, pick, (codebook, jnp.zeros_like(tokens)))
    diff = tokens.astype(F32) - quantized.astype(F32)
    token_loss = jnp.sum(diff * diff, axis=1) / width

    def add(step, carry):
        c, t, total, parts = carry
        owner = lax.rem(me - step + n, n)
        mine = (c // per_dev) == me
        total = total + jax.ops.segment_sum(
            jnp.where(mine, t, 0.0), c % per_dev, num_segments=per_dev
        )
        parts = lax.dynamic_update_slice(parts, jnp.sum(t)[None], (owner,))
        return lax.ppermute(c, AXES, ring), lax.ppermute(t, AXES, ring), total, parts

    start = (codes, token_loss, jnp.zeros((per_dev,), F32), jnp.zeros((n,), F32))
    _, _, code_loss, parts = lax.fori_loop(0, n, add, start)
    return quantized, token_loss, code_loss, 0.25 * jnp.sum(parts) / (rows * n)


def kernel(
    n, cols, cap, order_of,
    codes_ref, tokens_ref, book_ref,
    quant_ref, tloss_ref, counts_ref, closs_ref, commit_ref, perp_ref, flag_ref,
    csend, crecv, psend, precv, lsend, lrecv, ranks, low1h, sel,
    csem_s, csem_r, psem_s, psem_r, lsem_s, lsem_r,
):
    rows, width = tokens_ref.shape
    per = book_ref.shape[0]
    bits = per.bit_length() - 1
    total_tokens = rows * n
    my_row, my_col = lax.axis_index("row"), lax.axis_index("col")
    me = my_row * cols + my_col
    rows_at = [lax.rem(my_row + d, n // cols) for d in range(n // cols)]
    cols_at = [lax.rem(my_col + d, cols) for d in range(cols)]
    at = [(rows_at[k // cols], cols_at[k % cols]) for k in range(n)]
    peer = [r * cols + c for r, c in at]

    def copy(send, recv, ssem, rsem, k):
        return pltpu.make_async_remote_copy(
            src_ref=send.at[peer[k]],
            dst_ref=recv.at[me],
            send_sem=ssem.at[k],
            recv_sem=rsem.at[k],
            device_id=at[k],
            device_id_type=pl.DeviceIdType.MESH,
        )

    def start_all(*refs):
        for k in order_of:
            if k:
                copy(*refs, k).start()

    def wait_all(*refs):
        for k in order_of:
            if k:
                copy(*refs, k).wait_recv()

    def sent_all(*refs):
        for k in order_of:
            if k:
                copy(*refs, k).wait_send()

    barrier = pltpu.get_barrier_semaphore()
    for k in order_of:
        if k:
            pl.semaphore_signal(
                barrier, inc=1, device_id=at[k], device_id_type=pl.DeviceIdType.MESH
            )

    code_row = codes_ref[...].reshape(1, rows)
    hi_row = lax.shift_right_logical(code_row, bits)
    code_col = jnp.broadcast_to(code_row.astype(F32), (128, rows)).T.astype(jnp.int32)
    hi_col = lax.shift_right_logical(code_col, bits)
    lo_col = code_col & (per - 1)
    lane = lax.broadcasted_iota(jnp.int32, (rows, 128), 1)
    own_row = hi_row == lax.broadcasted_iota(jnp.int32, (n, rows), 0)
    for k in range(per // 128):
        low1h[:, k * 128 : (k + 1) * 128] = jnp.where(lo_col == lane + k * 128, 1.0, 0.0).astype(BF16)
    low = low1h[...]
    hist = jnp.dot(jnp.where(own_row, 1.0, 0.0).astype(BF16), low, preferred_element_type=F32)
    wanted = jnp.where(hist > 0.5, 1.0, 0.0)
    most = jnp.max(jnp.sum(wanted, axis=1, keepdims=True), axis=0, keepdims=True)
    most_wide = jnp.broadcast_to(most, (1, EXTRA))
    for p in range(n):
        csend[p, :, :per] = hist[p : p + 1, :]
        csend[p, :, per:] = most_wide
    crecv[pl.ds(me, 1)] = csend[pl.ds(me, 1)]

    pl.semaphore_wait(barrier, n - 1)
    start_all(csend, crecv, csem_s, csem_r)

    before = lax.broadcasted_iota(jnp.int32, (per, per), 0) < lax.broadcasted_iota(jnp.int32, (per, per), 1)
    before = jnp.where(before, 1.0, 0.0).astype(BF16)
    rank = jnp.dot(wanted.astype(BF16), before, preferred_element_type=F32)
    rank = jnp.minimum(rank, 255.0).astype(BF16)
    hi1h = jnp.where(hi_col[:, :n] == lane[:, :n], 1.0, 0.0).astype(BF16)
    looked = jnp.dot(hi1h, rank, preferred_element_type=F32).astype(BF16) * low
    found = jnp.dot(looked, jnp.ones((per, 128), BF16), preferred_element_type=F32)
    slot = hi_col * cap + found.astype(jnp.int32)
    for k in range(n * cap // 128):
        sel[:, k * 128 : (k + 1) * 128] = jnp.where(slot == lane + k * 128, 1.0, 0.0).astype(BF16)

    wait_all(csend, crecv, csem_s, csem_r)
    asked = crecv[:, 0, :per]
    present = asked > 0.5
    order = jnp.dot(jnp.where(present, 1.0, 0.0).astype(BF16), before, preferred_element_type=F32)
    order = jnp.where(present, order, -1.0)
    for p in range(n):
        ranks[p] = order[p : p + 1, :]

    place = lax.broadcasted_iota(jnp.int32, (cap, per), 0).astype(F32)
    book = book_ref[...]
    ready = []
    for g in range(0, n, GROUP):
        group = order_of[g : g + GROUP]
        picks = [
            jnp.where(jnp.broadcast_to(ranks[peer[k]], (cap, per)) == place, 1.0, 0.0).astype(BF16)
            for k in group
        ]
        packed = jnp.dot(jnp.concatenate(picks, axis=0), book, preferred_element_type=F32)
        packed = packed.astype(BF16)
        for i, k in enumerate(group):
            out = psend if k else precv
            out[peer[k]] = packed[i * cap : (i + 1) * cap]
        for k in ready:
            copy(psend, precv, psem_s, psem_r, k).start()
        ready = [k for k in group if k]
    for k in ready:
        copy(psend, precv, psem_s, psem_r, k).start()

    counts = jnp.sum(asked, axis=0, keepdims=True)
    counts_ref[...] = counts.astype(jnp.int32).reshape(per)
    probs = counts / total_tokens
    terms = jnp.where(
        counts > 0.5, probs * jnp.log(jnp.maximum(probs, 1.0 / total_tokens)), 0.0
    )
    entropy = jnp.sum(terms, axis=1, keepdims=True)
    flag_ref[0, 0] = jnp.max(crecv[:, 0, per:]).astype(jnp.int32)

    wait_all(psend, precv, psem_s, psem_r)
    packs = precv[...].reshape(n * cap, width)
    quant = jnp.dot(sel[...], packs, preferred_element_type=F32).astype(BF16)
    quant_ref[...] = quant
    diff = tokens_ref[...].astype(F32) - quant.astype(F32)
    square = diff * diff
    folded = square[:, :128]
    for k in range(1, width // 128):
        folded = folded + square[:, k * 128 : (k + 1) * 128]
    tloss = jnp.sum(folded.T, axis=0, keepdims=True) / width
    tloss_ref[...] = tloss.reshape(rows)
    part = jnp.sum(tloss, axis=1, keepdims=True)

    first = tloss.astype(BF16).astype(F32)
    second = (tloss - first).astype(BF16).astype(F32)
    third = tloss - first - second
    spread = jnp.concatenate(
        [jnp.where(own_row, x, 0.0).astype(BF16) for x in (first, second, third)], axis=0
    )
    sums = jnp.dot(spread, low1h[...], preferred_element_type=F32)
    sums = sums[:n] + sums[n : 2 * n] + sums[2 * n :]
    lane1 = lax.broadcasted_iota(jnp.int32, (1, EXTRA), 1)
    tail = jnp.where(lane1 == 0, part, jnp.where(lane1 == 1, entropy, 0.0))
    for p in range(n):
        lsend[p, :, :per] = sums[p : p + 1, :]
        lsend[p, :, per:] = tail
    lrecv[pl.ds(me, 1)] = lsend[pl.ds(me, 1)]
    start_all(lsend, lrecv, lsem_s, lsem_r)

    sent_all(csend, crecv, csem_s, csem_r)
    sent_all(psend, precv, psem_s, psem_r)
    wait_all(lsend, lrecv, lsem_s, lsem_r)
    added = jnp.sum(lrecv[:, 0, :], axis=0, keepdims=True)
    closs_ref[...] = added[:, :per].reshape(per)
    ends = added[:, per:]
    commit_ref[0, 0] = jnp.sum(jnp.where(lane1 == 0, ends, 0.0)) * (0.25 / total_tokens)
    perp = jnp.exp(-jnp.sum(jnp.where(lane1 == 1, ends, 0.0), axis=1, keepdims=True))
    perp_ref[0, 0] = jnp.max(jnp.broadcast_to(perp, (1, EXTRA)))
    sent_all(lsend, lrecv, lsem_s, lsem_r)


def send_order(n, cols):
    turns = sorted(range(n // cols), key=lambda d: (abs(2 * d - n // cols), d))
    turns = [d for d in turns if d] + [0]
    blocks = [(d, h) for d in turns for h in (0, 1)]
    half = cols // 2
    spread = sorted(blocks[2:-2], key=lambda b: b[1])
    blocks = blocks[:2] + spread + [(0, 1), (0, 0)]
    return [d * cols + h * half + c for d, h in blocks for c in range(half)]


def exchange(n, cols, cap, number, tokens, codebook, codes):
    rows, width = tokens.shape
    per = codebook.shape[0]
    vmem = pl.BlockSpec(memory_space=pltpu.VMEM)
    smem = pl.BlockSpec(memory_space=pltpu.SMEM)
    dma = pltpu.SemaphoreType.DMA((n,))
    message = pltpu.VMEM((n, 1, per + EXTRA), F32)
    return pl.pallas_call(
        functools.partial(kernel, n, cols, cap, send_order(n, cols)),
        out_shape=(
            jax.ShapeDtypeStruct((rows, width), BF16),
            jax.ShapeDtypeStruct((rows,), F32),
            jax.ShapeDtypeStruct((per,), jnp.int32),
            jax.ShapeDtypeStruct((per,), F32),
            jax.ShapeDtypeStruct((1, 1), F32),
            jax.ShapeDtypeStruct((1, 1), F32),
            jax.ShapeDtypeStruct((1, 1), jnp.int32),
        ),
        in_specs=[vmem] * 3,
        out_specs=(vmem, vmem, vmem, vmem, smem, smem, smem),
        scratch_shapes=[
            message, message,
            pltpu.VMEM((n, cap, width), BF16),
            pltpu.VMEM((n, cap, width), BF16),
            message, message,
            pltpu.VMEM((n, 1, per), F32),
            pltpu.VMEM((rows, per), BF16),
            pltpu.VMEM((rows, n * cap), BF16),
            dma, dma, dma, dma, dma, dma,
        ],
        compiler_params=pltpu.CompilerParams(collective_id=number, has_side_effects=True),
    )(codes, tokens, codebook)


def asked_plan(n, cols, cap, tokens, codebook, codes):
    rows = tokens.shape[0]
    per = codebook.shape[0]
    quantized, token_loss, counts, code_loss, commitment, perplexity, flag = exchange(
        n, cols, cap, 0, tokens, codebook, codes
    )

    def kept():
        return quantized, token_loss, code_loss, commitment[0, 0]

    def wider():
        q, t, _, c, m, _, _ = exchange(n, cols, 2 * cap, 1, tokens, codebook, codes)
        return q, t, c, m[0, 0]

    def any_codes():
        return lax.cond(
            flag[0, 0] > 2 * cap, lambda: ring_plan(n, tokens, codebook, codes), wider
        )

    quantized, token_loss, code_loss, commitment = lax.cond(flag[0, 0] > cap, any_codes, kept)
    return (
        quantized,
        token_loss,
        counts,
        code_loss,
        commitment,
        perplexity[0, 0],
    )


def on_device(n, cols, tokens, codebook, codes):
    rows, width = tokens.shape
    per = codebook.shape[0]
    cap = -(-rows // (n * 16)) * 16
    fits = (
        per % 128 == 0
        and per & (per - 1) == 0
        and rows % 128 == 0
        and width % 128 == 0
        and n * cap % 128 == 0
        and cols % 8 == 0
        and n // cols > 1
        and n <= 128
        and 2 * cap < min(per, 256)
    )
    if fits:
        return asked_plan(n, cols, cap, tokens, codebook, codes)
    return dense_plan(tokens, codebook, codes)


def solution(mesh):
    n = mesh.shape["row"] * mesh.shape["col"]
    return jax.shard_map(
        functools.partial(on_device, n, mesh.shape["col"]),
        mesh=mesh,
        in_specs=(P(AXES, None), P(AXES, None), P(AXES)),
        out_specs=(P(AXES, None), P(AXES), P(AXES), P(AXES), P(), P()),
        check_vma=False,
    )
```
